32 devices in a mesh: mom: 4 (over y, x), en: 8 (over z, core).
Axes of the slice: x: 2, y: 2, z: 4, core: 2. Of those that a mesh axis runs over, the one named last changes fastest.
Arguments:
- green_blocks: float32 [12, 8, 2, 512, 512], P('mom', 'en'), may hold values from -6 to 6
- transfer_index: int32 [12, 12], P('mom'), may hold values from 0 to 8
- photon_shift: int32 [12], P('mom'), may hold values from 1 to 2
- photon_occupancy: float32 [1], replicated, may hold values from 0.3 to 3
- coupling: bfloat16 [9, 512, 512], replicated, may hold values from -0.25 to 0.25
Outputs:
- self_energy: float32 [12, 8, 2, 512, 512], P('mom', 'en')
The draws below stay inside these ranges and needn't reach their ends.
All inputs are finite; a program needn't handle non-finite values.
Results may differ from the reference program's by a relative error of at most 0.0057.
Values may be sent and summed in bfloat16 or wider, within the bound.
No kernel may reach another device: no remote copies, remote signals or barrier semaphores. Data moves between devices by JAX's collectives and lax.ppermute only.
A program may use at most 192 MiB of HBM per device.

```python
import math
import jax
import jax.numpy as jnp
from jax import lax

NORB = 512
MOMENTA = 12
ENERGIES = 8
QC = 9


def set_ends(drawn, own_key, low, top_value):
    place = [jax.random.randint(jax.random.fold_in(own_key, axis), (), 0, length) for axis, length in enumerate(drawn.shape)]
    main_axis = drawn.shape.index(max(drawn.shape))
    next_to = place[:main_axis] + [(place[main_axis] + 1) % drawn.shape[main_axis]] + place[main_axis + 1:]
    return drawn.at[tuple(place)].set(low).at[tuple(next_to)].set(top_value)


def block_levels(own_key, extent, pieces, smallest, high):
    factor_of = 1.0
    for dim, blocks in pieces:
        heights = jax.random.uniform(jax.random.fold_in(jax.random.fold_in(own_key, 6), dim), (blocks,), jnp.float32, smallest / len(pieces), high / len(pieces))
        factor_of = factor_of * jnp.repeat(jnp.exp(heights), extent[dim] // blocks).reshape((-1,) + (1,) * (len(extent) - 1 - dim))
    return factor_of


def bell_draw(rng, shape, deviation, most, cuts=(), kind=jnp.bfloat16):
    values = deviation * jax.random.normal(rng, shape, jnp.float32)
    if cuts:
        values = values * block_levels(rng, shape, cuts, -0.22, 0.18)
    return jnp.clip(values, -most, most).astype(kind)


def setup_inputs(seed: int = 0) -> dict:
    arg_keys = jax.random.split(jax.random.key(seed), 6)
    green_blocks = bell_draw(arg_keys[0], (MOMENTA, ENERGIES, 2, NORB, NORB), 1.0, 6.0, ((0, 4), (1, 8)), jnp.float32)
    transfer_index = set_ends(jax.random.randint(arg_keys[1], (MOMENTA, MOMENTA), 0, QC), jax.random.fold_in(arg_keys[1], 1), 0, QC - 1).astype(jnp.int32)
    photon_shift = set_ends(jax.random.randint(arg_keys[2], (MOMENTA,), 1, 3), jax.random.fold_in(arg_keys[2], 1), 1, 2).astype(jnp.int32)
    photon_occupancy = jnp.clip(jnp.exp(jax.random.uniform(arg_keys[3], (1,), jnp.float32, math.log(0.3), math.log(3.0))), 0.3, 3.0)
    coupling = bell_draw(arg_keys[4], (QC, NORB, NORB), NORB ** -0.5, 0.25)
    return dict(green_blocks=green_blocks, transfer_index=transfer_index, photon_shift=photon_shift, photon_occupancy=photon_occupancy, coupling=coupling)


def reference(green_blocks, transfer_index, photon_shift, photon_occupancy, coupling):
    rounded = green_blocks.astype(jnp.bfloat16)
    padded = jnp.pad(rounded, ((0, 0), (2, 2), (0, 0), (0, 0), (0, 0)))
    near_mask = (photon_shift == 1)[:, None, None, None, None]
    below_rim = jnp.where(near_mask, padded[:, 1:1 + ENERGIES], padded[:, 0:ENERGIES])
    above_rim = jnp.where(near_mask, padded[:, 3:3 + ENERGIES], padded[:, 4:4 + ENERGIES])
    occupy = photon_occupancy[0]
    selector = (transfer_index[:, None, :] == jnp.arange(QC, dtype=jnp.int32)[None, :, None]).astype(jnp.float32)
    selector = selector.reshape(MOMENTA * QC, MOMENTA)
    weights = coupling.astype(jnp.float32)

    def one_energy(pair):
        below, above = pair
        mixed = (occupy * below.astype(jnp.float32) + (occupy + 1.0) * above.astype(jnp.float32)).astype(jnp.bfloat16)
        bins = jnp.dot(selector, mixed.astype(jnp.float32).reshape(MOMENTA, -1), precision=lax.Precision.HIGHEST)
        bins = bins.astype(jnp.bfloat16).reshape(MOMENTA, QC, 2, NORB, NORB)
        left = jnp.einsum('qxy,kqcyz->kqcxz', weights, bins.astype(jnp.float32), precision=lax.Precision.HIGHEST)
        left = left.astype(jnp.bfloat16)
        result = jnp.einsum('kqcxy,qzy->kcxz', left.astype(jnp.float32), weights, precision=lax.Precision.HIGHEST)
        return result / MOMENTA

    output = lax.map(one_energy, (jnp.moveaxis(below_rim, 1, 0), jnp.moveaxis(above_rim, 1, 0)))
    return jnp.moveaxis(output, 0, 1)
```

```python
import functools

import jax
import jax.numpy as jnp
from jax import lax
from jax.experimental import pallas as pl
from jax.experimental.pallas import tpu as pltpu
from jax.sharding import PartitionSpec as P


MEMBERS = 4
FIELDS = 8
UNROLL = 2
MIB = 1 << 20
LAST_ROWS = (((1,), (1,)), ((), ()))


def plan_kernel(sizes, own_ref, partner_ref, place_ref, table, count, member, filled):
    local, momenta, classes, bits, calls = sizes
    ways = 1 << bits
    slots = 2 * local * ways
    width = slots + MEMBERS
    bins = 2 * local * classes
    header = 2 * calls + 2

    def clear(i, _):
        count[i] = 0
        return 0

    lax.fori_loop(0, bins, clear, 0)

    def empty(i, _):
        member[i] = slots
        return 0

    lax.fori_loop(0, bins * width, empty, 0)

    def dummy(i, _):
        field = lax.rem(i, FIELDS)
        table[header + i] = jnp.where(field < 2, 0, slots)
        return 0

    lax.fori_loop(0, table.shape[0] - header, dummy, 0)
    for call in range(calls + 1):
        filled[call] = 0

    def sort_slot(slot, _):
        stage = lax.div(slot, ways)
        way = lax.rem(slot, ways)
        home = place_ref[0]
        for bit in range(bits):
            home = home ^ jnp.where((way >> bit) & 1 == 1, place_ref[2 + bit], 0)
        home = home ^ jnp.where(stage < local, place_ref[1], 0)
        momentum = home * local + lax.rem(stage, local)
        for k in range(2 * local):
            of_k = partner_ref[k, momentum] if k < local else own_ref[k - local, momentum]
            index = k * classes + of_k
            have = count[index]
            member[index * width + have] = slot
            count[index] = have + 1
        return 0

    lax.fori_loop(0, slots, sort_slot, 0)

    def each_job(act):
        def one_bin(index, _):
            k = lax.div(index, classes)
            have = count[index]

            def one_job(j, _):
                first = index * width + j * MEMBERS
                latest = member[index * width + jnp.minimum(j * MEMBERS + MEMBERS, have) - 1]
                stage = lax.div(latest, ways)
                call = stage + jnp.where((stage == 2 * local - 1) & (k >= local), 1, 0)
                act(call, k, index - k * classes, first)
                return 0

            return lax.fori_loop(0, lax.div(have + MEMBERS - 1, MEMBERS), one_job, 0)

        lax.fori_loop(0, bins, one_bin, 0)

    def tally(call, k, q, first):
        filled[call] = filled[call] + 1

    each_job(tally)
    start = 0
    for call in range(calls):
        steps = lax.div(filled[call] + UNROLL - 1, UNROLL)
        table[2 * call] = start
        table[2 * call + 1] = steps
        filled[call] = start
        start = start + steps * UNROLL

    def write(call, k, q, first):
        place = filled[call]
        filled[call] = place + 1
        at = header + place * FIELDS
        table[at] = k
        table[at + 1] = q
        for i in range(MEMBERS):
            table[at + 2 + i] = member[first + i]

    each_job(write)


def stage_kernel(call, calls, arrived, scale, table, coupling, *refs):
    parts = refs[:arrived]
    first_call = call == 0
    refs = refs[arrived:] if first_call else refs[arrived + 2 :]
    blocks, total = refs[:2]
    send = refs[2] if len(refs) > 2 else None
    slots = blocks.shape[0] - 1
    if first_call:
        blocks[slots] = jnp.zeros(blocks.shape[1:], blocks.dtype)
        total[...] = jnp.zeros(total.shape, total.dtype)
    if arrived:
        ways = sum(part.shape[0] for part in parts)
        at = call * ways
        for part in parts:
            for i in range(part.shape[0]):
                blocks[at] = part[i]
                at += 1
    start = table[2 * call]
    header = 2 * calls + 2

    def step(i, _):
        for u in range(UNROLL):
            at = header + (start + i * UNROLL + u) * FIELDS
            k, q = table[at], table[at + 1]
            summed = blocks[table[at + 2]].astype(jnp.float32)
            for j in range(1, MEMBERS):
                summed = summed + blocks[table[at + 2 + j]].astype(jnp.float32)
            weight = coupling[q]
            left = jnp.dot(weight, summed.astype(blocks.dtype), preferred_element_type=jnp.float32)
            total[k] += lax.dot_general(
                left.astype(blocks.dtype), weight, LAST_ROWS, preferred_element_type=jnp.float32
            )
        return 0

    lax.fori_loop(0, table[2 * call + 1], step, 0)
    if send is not None:
        for k in range(send.shape[0]):
            send[k] = (total[k] * scale).astype(send.dtype)


def write_own_kernel(scale, part_ref, total, out):
    out[0, 0, 0] = total[0] * scale


def write_other_kernel(part_ref, got, whole, out):
    out[0, 0, 0] = got[0].astype(out.dtype)


def solution(mesh):
    moms, energies = mesh.shape["mom"], mesh.shape["en"]
    bits = moms.bit_length() - 2
    top = moms // 2
    both = ("mom", "en")

    def move(value, target):
        pairs = []
        for m in range(moms):
            for e in range(energies):
                to_m, to_e = target(m, e)
                if not 0 <= to_e < energies:
                    to_m, to_e = m, e ^ 1
                pairs.append((m * energies + e, to_m * energies + to_e))
        return lax.ppermute(value, both, pairs)

    def away(m, e):
        return m, e + (2 if e % 2 else -2)

    def toward(m, e):
        return m, e + (-2 if e % 2 else 2)

    def core_mate(m, e):
        return m, e ^ 1

    def partner(m, e):
        return m ^ (top if e % 2 else 1), e

    def gather_bit(bit):
        return lambda m, e: (m ^ ((1 << bit) if e % 2 else (2 << bit)), e)

    def body(green_blocks, transfer_index, photon_shift, photon_occupancy, coupling):
        local, _, parts, orbitals, _ = green_blocks.shape
        momenta = transfer_index.shape[1]
        classes = coupling.shape[0]
        ways = 1 << bits
        slots = 2 * local * ways
        calls = 2 * local + 1
        low = jnp.bfloat16
        scale = 1.0 / momenta
        m, e = lax.axis_index("mom"), lax.axis_index("en")
        core = e % 2
        bit_of = (m & 1, (m // top) & 1)
        mine = jnp.where(core == 0, bit_of[0], bit_of[1])
        mates = jnp.where(core == 0, bit_of[1], bit_of[0])
        flat = green_blocks.reshape(local, parts, orbitals, orbitals)

        def part_of(which):
            return lax.dynamic_index_in_dim(flat, which, 1, keepdims=False).astype(low)

        partner_index = move(transfer_index, partner)
        place = jnp.stack(
            [m, jnp.where(core == 0, 1, top)]
            + [jnp.where(core == 0, 2 << bit, 1 << bit) for bit in range(bits)]
        ).astype(jnp.int32)
        bins = 2 * local * classes
        smem = pl.BlockSpec(memory_space=pltpu.SMEM)
        vmem = pl.BlockSpec(memory_space=pltpu.VMEM)
        room = 2 * calls + 2 + (2 * local * momenta + UNROLL * calls) * FIELDS
        table = pl.pallas_call(
            functools.partial(plan_kernel, (local, momenta, classes, bits, calls)),
            in_specs=[smem] * 3,
            out_specs=smem,
            out_shape=jax.ShapeDtypeStruct((room,), jnp.int32),
            scratch_shapes=[
                pltpu.SMEM((bins,), jnp.int32),
                pltpu.SMEM((bins * (slots + MEMBERS),), jnp.int32),
                pltpu.SMEM((calls + 1,), jnp.int32),
            ],
            name="plan",
        )(transfer_index, partner_index, place)

        near = photon_shift == 1
        occupy = photon_occupancy[0]
        has_below, has_above = e >= 2, e + 2 < energies
        even = core == 0
        weight_toward = jnp.where(even, occupy, occupy + 1.0) * jnp.where(
            jnp.where(even, has_below, has_above), 1.0, 0.0
        )
        weight_away = jnp.where(even, occupy + 1.0, occupy) * jnp.where(
            near | jnp.where(even, has_above, has_below), 1.0, 0.0
        )

        def mixed_units(which, mates_which):
            block = part_of(which)
            gone = move(block, away)
            mate = move(part_of(mates_which), core_mate)
            units = []
            for k in range(local):
                chosen = jnp.where(near[k], mate[k], block[k])[None]
                came = move(chosen, toward)
                other = jnp.where(near[k], mate[k], gone[k])[None]
                units.append(
                    (
                        weight_toward * came.astype(jnp.float32)
                        + weight_away[k] * other.astype(jnp.float32)
                    ).astype(low)
                )
            return units

        for_partner = mixed_units(1 - mine, 1 - mates)
        own = mixed_units(mine, mates)
        stages = [move(unit, partner) for unit in for_partner] + own

        weights = pltpu.with_memory_space_constraint(coupling, pltpu.VMEM)
        state = None
        block_shape = (orbitals, orbitals)
        out_state = [
            pltpu.VMEM((slots + 1, *block_shape), low),
            pltpu.VMEM((2 * local, *block_shape), jnp.float32),
        ]
        params = pltpu.CompilerParams(vmem_limit_bytes=14 * MIB)
        product = 4 * orbitals**3

        def stage(call, arrived, state, sends, jobs):
            given = [] if state is None else list(state)
            result = pl.pallas_call(
                functools.partial(stage_kernel, call, calls, len(arrived), scale),
                in_specs=[smem, vmem] + [vmem] * (len(arrived) + len(given)),
                out_specs=[vmem] * (2 + sends),
                out_shape=out_state
                + [jax.ShapeDtypeStruct((local, *block_shape), low)] * sends,
                input_output_aliases={2 + len(arrived) + i: i for i in range(len(given))},
                compiler_params=params,
                cost_estimate=pl.CostEstimate(
                    flops=jobs * product, bytes_accessed=MIB, transcendentals=0
                ),
                name=f"stage_{call}",
            )(table, weights, *arrived, *given)
            return result[:2], result[2:]

        sent = ()
        for call, unit in enumerate(stages):
            arrived = [unit]
            held = unit
            for bit in range(bits):
                came = move(held, gather_bit(bit))
                arrived.append(came)
                if bit + 1 < bits:
                    held = jnp.concatenate([held, came])
            state, sent = stage(call, arrived, state, int(call == 2 * local - 1), 6)
        got = move(sent[0], partner)
        state, _ = stage(2 * local, [], state, 0, 6)

        out_shape = jax.ShapeDtypeStruct(green_blocks.shape, jnp.float32)
        part_block = (1, 1, 1, *block_shape)
        half = pl.pallas_call(
            functools.partial(write_own_kernel, scale),
            grid_spec=pltpu.PrefetchScalarGridSpec(
                num_scalar_prefetch=1,
                grid=(local,),
                in_specs=[pl.BlockSpec((1, *block_shape), lambda i, p: (local + i, 0, 0))],
                out_specs=pl.BlockSpec(part_block, lambda i, p: (i, 0, p[0], 0, 0)),
            ),
            out_shape=out_shape,
            compiler_params=pltpu.CompilerParams(vmem_limit_bytes=8 * MIB),
            name="write_own",
        )(mine.reshape(1), state[1])
        return pl.pallas_call(
            write_other_kernel,
            grid_spec=pltpu.PrefetchScalarGridSpec(
                num_scalar_prefetch=1,
                grid=(local,),
                in_specs=[
                    pl.BlockSpec((1, *block_shape), lambda i, p: (i, 0, 0)),
                    pl.BlockSpec(memory_space=pl.ANY),
                ],
                out_specs=pl.BlockSpec(part_block, lambda i, p: (i, 0, p[0], 0, 0)),
            ),
            out_shape=out_shape,
            input_output_aliases={2: 0},
            compiler_params=pltpu.CompilerParams(vmem_limit_bytes=8 * MIB),
            name="write_other",
        )((1 - mine).reshape(1), got, half)

    placed = (P("mom", "en", None, None, None), P("mom", None), P("mom"), P(), P())
    return jax.shard_map(
        body,
        mesh=mesh,
        in_specs=placed,
        out_specs=P("mom", "en", None, None, None),
        check_vma=False,
    )
```

```python
import functools

import jax
import jax.numpy as jnp
from jax import lax
from jax.experimental import pallas as pl
from jax.experimental.pallas import tpu as pltpu
from jax.sharding import PartitionSpec as P


MEMBERS = 4
FIELDS = 8
SIZES = (4, 2, 1)
MIB = 1 << 20
LAST_ROWS = (((1,), (1,)), ((), ()))


def pieces_of(local):
    return [1] * (2 * local - 1) + [2]


def settle(near, occupancy, place, weights):
    local = len(near)
    occupy = occupancy[0]
    even, has_toward, has_away = place[0] == 1, place[1] == 1, place[2] == 1
    weights[0] = jnp.where(has_toward, jnp.where(even, occupy, occupy + 1.0), 0.0)
    heavy = jnp.where(even, occupy + 1.0, occupy)
    for k in range(local):
        weights[1 + k] = jnp.where(near[k], heavy, 0.0)
        weights[1 + local + k] = jnp.where(near[k] | jnp.logical_not(has_away), 0.0, heavy)


def plan_kernel(sizes, own_ref, partner_ref, occupancy, sides, place_ref, table, weights, count, member, filled):
    local, momenta, classes, bits, calls = sizes
    ways = 1 << bits
    slots = 2 * local * ways
    bins = 2 * local * classes
    room = 2 * local * momenta
    near = [lax.div(partner_ref[k, 0], classes) == 1 for k in range(local)]
    settle(near, occupancy, sides, weights)

    for index in range(bins):
        count[index] = 0
    for call in range(calls):
        filled[call] = 0
        table[call] = 0

    def sort_slot(slot, _):
        stage = lax.div(slot, ways)
        way = lax.rem(slot, ways)
        home = place_ref[0]
        for bit in range(bits):
            home = home ^ jnp.where((way >> bit) & 1 == 1, place_ref[2 + bit], 0)
        home = home ^ jnp.where(stage < local, 0, place_ref[1])
        momentum = home * local + lax.rem(stage, local)
        for k in range(2 * local):
            of_k = partner_ref[k, momentum] if k < local else own_ref[k - local, momentum]
            of_k = lax.rem(of_k, classes)
            index = k * classes + of_k
            have = count[index]
            member[index * slots + have] = slot
            count[index] = have + 1
        return 0

    lax.fori_loop(0, slots, sort_slot, 0)

    for k in range(2 * local):

        def one_bin(q, _):
            index = k * classes + q
            have = count[index]

            def one_job(j, _):
                first = index * slots + j * MEMBERS
                upto = jnp.minimum(MEMBERS, have - j * MEMBERS)
                stage = lax.div(member[first + upto - 1], ways)
                last = 2 * local - 1
                call = jnp.where(stage == last, last + 1 + min(k, local), stage)
                if k >= local:
                    call = jnp.where(stage == last - 1, last, call)
                place = filled[call]
                filled[call] = place + 1
                table[call] = place + 1
                at = calls + (call * room + place) * FIELDS
                table[at] = k
                table[at + 1] = q
                for i in range(MEMBERS):
                    table[at + 2 + i] = jnp.where(i < upto, member[first + i], slots)
                return 0

            return lax.fori_loop(0, lax.div(have + MEMBERS - 1, MEMBERS), one_job, 0)

        lax.fori_loop(0, classes, one_bin, 0)


def convert_first_kernel(part_ref, block, out):
    out[0] = block[0, 0].astype(out.dtype)


def convert_kernel(local, part_ref, shift, occupancy, sides, block, *outs):
    step = pl.program_id(0)
    low = outs[0].dtype
    weights, flags = outs[-2:]

    @pl.when(step == 0)
    def _():
        near = [shift[k] == 1 for k in range(local)]
        settle(near, occupancy, sides, weights)
        for k in range(local):
            flags[k] = jnp.where(near[k], 1, 0)

    for k in range(1, local):

        @pl.when(step == k)
        def _():
            outs[k - 1][0] = block[0, part_ref[0]].astype(low)

    outs[local - 1][step] = block[0, part_ref[1]].astype(low)
    outs[local][step] = block[0, part_ref[2]].astype(low)
    outs[local][local + step] = block[0, part_ref[3]].astype(low)


def choose_kernel(local, flags, mate, *refs):
    own, others, outs = refs[:local], refs[local], list(refs[local + 1 :])
    for k, cuts in enumerate(pieces_of(local)):
        rows = mate.shape[1] // cuts
        given, at = (own[k], 0) if k < local else (others, k - local)
        near = flags[k % local] == 1
        for top in range(0, mate.shape[1], rows):
            out = outs.pop(0)

            @pl.when(near)
            def _():
                out[0] = mate[k, top : top + rows]

            @pl.when(jnp.logical_not(near))
            def _():
                out[0] = given[at, top : top + rows]


def mix_kernel(k, local, weights, came, chosen, gone, out):
    wide = jnp.float32
    out[...] = (
        weights[0] * came[...].astype(wide)
        + (
            weights[1 + k] * chosen[...].astype(wide)
            + weights[1 + local + k] * gone[...].astype(wide)
        )
    ).astype(out.dtype)


def run_jobs(call, calls, table, coupling, blocks, total, wide=False):
    header = calls + call * ((table.shape[0] - calls) // calls)

    def step(i, _, first, jobs):
        for u in range(jobs):
            at = header + (first + i * jobs + u) * FIELDS
            k, q = table[at], table[at + 1]
            summed = blocks[table[at + 2]].astype(jnp.float32)
            for j in range(1, MEMBERS):
                summed = summed + blocks[table[at + 2 + j]].astype(jnp.float32)
            weight = coupling[q]
            left = jnp.dot(weight, summed.astype(blocks.dtype), preferred_element_type=jnp.float32)
            total[k] += lax.dot_general(
                left.astype(blocks.dtype), weight, LAST_ROWS, preferred_element_type=jnp.float32
            )
        return 0

    done, jobs = 0, table[call]
    for size in SIZES[0 if wide else 1 :]:
        count = lax.div(jobs - done, size)
        lax.fori_loop(0, count, functools.partial(step, first=done, jobs=size), 0)
        done = done + count * size


def stage_kernel(call, calls, base, ways, arrived, sends, scale, table, coupling, *refs):
    parts = refs[:arrived]
    first_call = call == 0
    refs = refs[arrived:] if first_call else refs[arrived + 2 :]
    blocks, total = refs[:2]
    send = refs[2] if len(refs) > 2 else None
    slots = blocks.shape[0] - 1
    if first_call:
        blocks[slots] = jnp.zeros(blocks.shape[1:], blocks.dtype)
        total[...] = jnp.zeros(total.shape, total.dtype)
    for way in range(ways if arrived else 0):
        top = 0
        for part in parts[way * arrived // ways : (way + 1) * arrived // ways]:
            rows = part.shape[1]
            blocks[base + way, top : top + rows] = part[0]
            top += rows
    run_jobs(call, calls, table, coupling, blocks, total)
    if send is not None:
        for i, k in enumerate(sends):
            send[i] = (total[k] * scale).astype(send.dtype)


def finish_kernel(call, calls, scale, table, part_ref, coupling, blocks, total_in, total, out, ready, done):
    run_jobs(call, calls, table, coupling, blocks, total, wide=True)
    local = ready.shape[0]
    copies = []
    for k in range(local):
        ready[k] = total[local + k] * scale
        copies.append(pltpu.make_async_copy(ready.at[k], out.at[k, 0, part_ref[0]], done.at[k]))
        copies[k].start()
    for copy in copies:
        copy.wait()


def write_other_kernel(at, part_ref, *refs):
    parts, (out, ready, done) = refs[:-4], refs[-3:]
    copies = []
    for k, part in enumerate(parts):
        ready[k] = part[0].astype(ready.dtype)
        place = out.at[at + k, 0, part_ref[0]]
        copies.append(pltpu.make_async_copy(ready.at[k], place, done.at[k]))
        copies[k].start()
    for copy in copies:
        copy.wait()


def solution(mesh):
    moms, energies = mesh.shape["mom"], mesh.shape["en"]
    bits = moms.bit_length() - 2
    top = moms // 2
    both = ("mom", "en")

    def move(value, target):
        pairs = []
        for m in range(moms):
            for e in range(energies):
                to_m, to_e = target(m, e)
                if not 0 <= to_e < energies:
                    to_m, to_e = m, e ^ 1
                pairs.append((m * energies + e, to_m * energies + to_e))
        return lax.ppermute(value, both, pairs)

    def away(m, e):
        return m, e + (2 if e % 2 else -2)

    def toward(m, e):
        return m, e + (-2 if e % 2 else 2)

    def core_mate(m, e):
        return m, e ^ 1

    def partner(m, e):
        return m ^ (top if e % 2 else 1), e

    def gather_bit(bit):
        return lambda m, e: (m ^ ((1 << bit) if e % 2 else (2 << bit)), e)

    def body(green_blocks, transfer_index, photon_shift, photon_occupancy, coupling):
        local, _, parts, orbitals, _ = green_blocks.shape
        momenta = transfer_index.shape[1]
        classes = coupling.shape[0]
        ways = 1 << bits
        slots = 2 * local * ways
        last = 2 * local - 1
        calls = last + local + 2
        low = jnp.bfloat16
        scale = 1.0 / momenta
        m, e = lax.axis_index("mom"), lax.axis_index("en")
        even = e % 2 == 0
        bit_of = (m & 1, (m // top) & 1)
        mine = jnp.where(even, bit_of[0], bit_of[1])
        mates = jnp.where(even, bit_of[1], bit_of[0])
        flat = green_blocks.reshape(local, parts, orbitals, orbitals)
        block_shape = (orbitals, orbitals)
        smem = pl.BlockSpec(memory_space=pltpu.SMEM)
        vmem = pl.BlockSpec(memory_space=pltpu.VMEM)
        product = 4 * orbitals**3
        pieces = pieces_of(local)

        def kernel(act, *args, flops=1 << 20, vmem_mib=8, **more):
            return pl.pallas_call(
                act,
                compiler_params=pltpu.CompilerParams(vmem_limit_bytes=vmem_mib * MIB),
                cost_estimate=pl.CostEstimate(flops=flops, bytes_accessed=MIB, transcendentals=0),
                **more,
            )(*args)

        def send(value, target):
            came = move(value, target)
            if value.dtype != low:
                return came
            return pltpu.with_memory_space_constraint(came, pltpu.VMEM)

        place = jnp.stack(
            [m, jnp.where(even, 1, top)]
            + [jnp.where(even, 2 << bit, 1 << bit) for bit in range(bits)]
        ).astype(jnp.int32)
        has_below, has_above = e >= 2, e + 2 < energies
        sides = jnp.stack(
            [even, jnp.where(even, has_below, has_above), jnp.where(even, has_above, has_below)]
        ).astype(jnp.int32)
        which = jnp.stack([mine, 1 - mine, mates, 1 - mates]).astype(jnp.int32)
        place, sides, which = lax.optimization_barrier((place, sides, which))
        packed = transfer_index + classes * photon_shift[:, None]
        partner_index = send(packed, partner)

        flat = pltpu.with_memory_space_constraint(flat, pltpu.HBM)
        near_unit = pltpu.VMEM((1, *block_shape), low)
        near_units = pltpu.VMEM((local, *block_shape), low)
        weight_count = pltpu.SMEM((1 + 2 * local,), jnp.float32)
        first = kernel(
            convert_first_kernel,
            which,
            flat,
            grid_spec=pltpu.PrefetchScalarGridSpec(
                num_scalar_prefetch=1,
                grid=(1,),
                in_specs=[pl.BlockSpec((1, 1, *block_shape), lambda i, p: (0, p[0], 0, 0))],
                out_specs=vmem,
            ),
            out_shape=near_unit,
        )
        *rounded, own_weights, flags = kernel(
            functools.partial(convert_kernel, local),
            which,
            photon_shift,
            photon_occupancy,
            sides,
            flat,
            grid_spec=pltpu.PrefetchScalarGridSpec(
                num_scalar_prefetch=1,
                grid=(local,),
                in_specs=[smem] * 3
                + [pl.BlockSpec((1, parts, *block_shape), lambda i, p: (i, 0, 0, 0))],
                out_specs=[vmem] * (local + 1) + [smem] * 2,
            ),
            out_shape=[near_unit] * (local - 1)
            + [near_units, pltpu.VMEM((2 * local, *block_shape), low)]
            + [weight_count, pltpu.SMEM((local,), jnp.int32)],
        )
        own, (others, mates_blocks) = [first, *rounded[: local - 1]], rounded[local - 1 :]
        mate = send(mates_blocks, core_mate)
        ready = kernel(
            functools.partial(choose_kernel, local),
            flags,
            mate,
            *own,
            others,
            in_specs=[smem] + [vmem] * (2 + local),
            out_specs=[vmem] * sum(pieces),
            out_shape=[
                pltpu.VMEM((1, orbitals // n, orbitals), low) for n in pieces for _ in range(n)
            ],
        )
        ready = list(ready)
        ready = [[ready.pop(0) for _ in range(n)] for n in pieces]

        def sends(values, target):
            return [send(value, target) for value in values]

        gone = [sends([own[k]], away) for k in range(local)]
        chosen = ready[:local]
        chosen += [sends(ready[k], partner) for k in range(local, 2 * local)]
        gone += [sends(chosen[k], away) for k in range(local, 2 * local)]
        came = [sends(value, toward) for value in chosen]
        bins = 2 * local * classes
        room = calls + calls * 2 * local * momenta * FIELDS
        table, partner_weights = kernel(
            functools.partial(plan_kernel, (local, momenta, classes, bits, calls)),
            packed,
            partner_index,
            photon_occupancy,
            sides,
            place,
            in_specs=[smem] * 5,
            out_specs=[smem] * 2,
            out_shape=[pltpu.SMEM((room,), jnp.int32), weight_count],
            scratch_shapes=[
                pltpu.SMEM((bins,), jnp.int32),
                pltpu.SMEM((bins * slots,), jnp.int32),
                pltpu.SMEM((calls,), jnp.int32),
            ],
        )

        stages = [
            [
                kernel(
                    functools.partial(mix_kernel, k % local, local),
                    own_weights if k < local else partner_weights,
                    came[k][i],
                    chosen[k][i],
                    gone[k][i],
                    in_specs=[smem] + [vmem] * 3,
                    out_specs=vmem,
                    out_shape=pltpu.VMEM(came[k][i].shape, low),
                )
                for i in range(pieces[k])
            ]
            for k in range(2 * local)
        ]

        weights = pltpu.with_memory_space_constraint(coupling, pltpu.VMEM)
        out_state = [
            pltpu.VMEM((slots + 1, *block_shape), low),
            pltpu.VMEM((2 * local, *block_shape), jnp.float32),
        ]

        def stage(call, arrived, state, sends, jobs, base=0):
            given = [] if state is None else list(state)
            result = kernel(
                functools.partial(stage_kernel, call, calls, base, ways, len(arrived), sends, scale),
                table,
                weights,
                *arrived,
                *given,
                flops=jobs * product,
                vmem_mib=12,
                in_specs=[smem, vmem] + [vmem] * (len(arrived) + len(given)),
                out_specs=[vmem] * (2 + bool(sends)),
                out_shape=out_state + [pltpu.VMEM((len(sends), *block_shape), low)] * bool(sends),
                input_output_aliases={2 + len(arrived) + i: i for i in range(len(given))},
            )
            return result[:2], result[2:]

        state = None
        got = []
        for call, held in enumerate(stages):
            arrived = [held]
            for bit in range(bits):
                for values in list(arrived):
                    arrived.append(sends(values, gather_bit(bit)))
            arrived = [piece for values in arrived for piece in values]
            sends_now = [0] if call == last else []
            state, sent = stage(call + (call == last), arrived, state, sends_now, 5, call * ways)
        got = []
        for k in range(local):
            if k:
                state, sent = stage(last + 1 + k, [], state, [k], 2)
            got.append(send(sent[0], partner))
        state, _ = stage(last, [], state, [], 5)

        hbm = pl.BlockSpec(memory_space=pltpu.HBM)
        out_shape = jax.ShapeDtypeStruct(green_blocks.shape, jnp.float32)
        staging = [
            pltpu.VMEM((local, *block_shape), jnp.float32),
            pltpu.SemaphoreType.DMA((local,)),
        ]
        _, result = kernel(
            functools.partial(finish_kernel, last + 1 + local, calls, scale),
            table,
            mine.reshape(1),
            weights,
            *state,
            vmem_mib=14,
            in_specs=[smem] * 2 + [vmem] * 3,
            out_specs=[vmem, hbm],
            out_shape=[out_state[1], out_shape],
            input_output_aliases={4: 0},
            scratch_shapes=staging,
        )
        for name, values in (("early", got[:-1]), ("last", got[-1:])):
            result = kernel(
                functools.partial(write_other_kernel, 0 if name == "early" else local - 1),
                (1 - mine).reshape(1),
                *values,
                result,
                in_specs=[smem] + [vmem] * len(values) + [hbm],
                out_specs=hbm,
                out_shape=out_shape,
                input_output_aliases={1 + len(values): 0},
                scratch_shapes=staging,
            )
        return result

    placed = (P("mom", "en", None, None, None), P("mom", None), P("mom"), P(), P())

    return jax.shard_map(
        body,
        mesh=mesh,
        in_specs=placed,
        out_specs=P("mom", "en", None, None, None),
        check_vma=False,
    )
```

```python
import functools

import jax
import jax.numpy as jnp
from jax import lax
from jax.experimental import pallas as pl
from jax.experimental.pallas import tpu as pltpu
from jax.sharding import PartitionSpec as P


MEMBERS = 4
FIELDS = 8
SIZES = (4, 2, 1)
MIB = 1 << 20
LAST_ROWS = (((1,), (1,)), ((), ()))


def pieces_of(local):
    return [1] * (2 * local - 1) + [2]


def settle(near, occupancy, place, weights):
    local = len(near)
    occupy = occupancy[0]
    even, has_toward, has_away = place[0] == 1, place[1] == 1, place[2] == 1
    weights[0] = jnp.where(has_toward, jnp.where(even, occupy, occupy + 1.0), 0.0)
    heavy = jnp.where(even, occupy + 1.0, occupy)
    for k in range(local):
        weights[1 + k] = jnp.where(near[k], heavy, 0.0)
        weights[1 + local + k] = jnp.where(near[k] | jnp.logical_not(has_away), 0.0, heavy)


def plan_kernel(sizes, own_ref, partner_ref, occupancy, sides, place_ref, table, weights, count, member, filled):
    local, momenta, classes, bits, calls = sizes
    ways = 1 << bits
    slots = 2 * local * ways
    bins = 2 * local * classes
    room = 2 * local * momenta
    near = [lax.div(partner_ref[k, 0], classes) == 1 for k in range(local)]
    settle(near, occupancy, sides, weights)

    for index in range(bins):
        count[index] = 0
    for call in range(calls):
        filled[call] = 0
        table[call] = 0

    def sort_slot(slot, _):
        stage = lax.div(slot, ways)
        way = lax.rem(slot, ways)
        home = place_ref[0]
        for bit in range(bits):
            home = home ^ jnp.where((way >> bit) & 1 == 1, place_ref[2 + bit], 0)
        home = home ^ jnp.where(stage < local, 0, place_ref[1])
        momentum = home * local + lax.rem(stage, local)
        for k in range(2 * local):
            of_k = partner_ref[k, momentum] if k < local else own_ref[k - local, momentum]
            of_k = lax.rem(of_k, classes)
            index = k * classes + of_k
            have = count[index]
            member[index * slots + have] = slot
            count[index] = have + 1
        return 0

    lax.fori_loop(0, slots, sort_slot, 0)

    for k in range(2 * local):

        def one_bin(q, _):
            index = k * classes + q
            have = count[index]

            def one_job(j, _):
                first = index * slots + j * MEMBERS
                upto = jnp.minimum(MEMBERS, have - j * MEMBERS)
                stage = lax.div(member[first + upto - 1], ways)
                last = 2 * local - 1
                call = jnp.where(stage == last, last + 2 + min(k, local), stage)
                if k >= local:
                    call = call + jnp.where((stage == last - 1) | (stage == last - 2), 2, 0)
                place = filled[call]
                filled[call] = place + 1
                table[call] = place + 1
                at = calls + (call * room + place) * FIELDS
                table[at] = k
                table[at + 1] = q
                for i in range(MEMBERS):
                    table[at + 2 + i] = jnp.where(i < upto, member[first + i], slots)
                return 0

            return lax.fori_loop(0, lax.div(have + MEMBERS - 1, MEMBERS), one_job, 0)

        lax.fori_loop(0, classes, one_bin, 0)


def convert_first_kernel(part_ref, block, out):
    out[0] = block[0, 0].astype(out.dtype)


def convert_kernel(local, part_ref, shift, occupancy, sides, block, *outs):
    step = pl.program_id(0)
    low = outs[0].dtype
    weights, flags = outs[-2:]

    @pl.when(step == 0)
    def _():
        near = [shift[k] == 1 for k in range(local)]
        settle(near, occupancy, sides, weights)
        for k in range(local):
            flags[k] = jnp.where(near[k], 1, 0)

    for k in range(1, local):

        @pl.when(step == k)
        def _():
            outs[k - 1][0] = block[0, part_ref[0]].astype(low)

    outs[local - 1][step] = block[0, part_ref[1]].astype(low)
    outs[local][step] = block[0, part_ref[2]].astype(low)
    outs[local][local + step] = block[0, part_ref[3]].astype(low)


def choose_kernel(local, flags, mate, *refs):
    own, others, outs = refs[:local], refs[local], list(refs[local + 1 :])
    for k, cuts in enumerate(pieces_of(local)):
        rows = mate.shape[1] // cuts
        given, at = (own[k], 0) if k < local else (others, k - local)
        near = flags[k % local] == 1
        for top in range(0, mate.shape[1], rows):
            out = outs.pop(0)

            @pl.when(near)
            def _():
                out[0] = mate[k, top : top + rows]

            @pl.when(jnp.logical_not(near))
            def _():
                out[0] = given[at, top : top + rows]


def mix_kernel(k, local, weights, came, chosen, gone, out):
    wide = jnp.float32
    out[...] = (
        weights[0] * came[...].astype(wide)
        + (
            weights[1 + k] * chosen[...].astype(wide)
            + weights[1 + local + k] * gone[...].astype(wide)
        )
    ).astype(out.dtype)


def run_jobs(call, calls, table, coupling, blocks, total, wide=False):
    header = calls + call * ((table.shape[0] - calls) // calls)

    def step(i, _, first, jobs):
        for u in range(jobs):
            at = header + (first + i * jobs + u) * FIELDS
            k, q = table[at], table[at + 1]
            summed = blocks[table[at + 2]].astype(jnp.float32)
            for j in range(1, MEMBERS):
                summed = summed + blocks[table[at + 2 + j]].astype(jnp.float32)
            weight = coupling[q]
            left = jnp.dot(weight, summed.astype(blocks.dtype), preferred_element_type=jnp.float32)
            total[k] += lax.dot_general(
                left.astype(blocks.dtype), weight, LAST_ROWS, preferred_element_type=jnp.float32
            )
        return 0

    done, jobs = 0, table[call]
    for size in SIZES[0 if wide else 1 :]:
        count = lax.div(jobs - done, size)
        lax.fori_loop(0, count, functools.partial(step, first=done, jobs=size), 0)
        done = done + count * size


def stage_kernel(call, calls, base, ways, arrived, sends, scale, table, coupling, *refs):
    parts = refs[:arrived]
    first_call = call == 0
    refs = refs[arrived:] if first_call else refs[arrived + 2 :]
    blocks, total = refs[:2]
    send = refs[2] if len(refs) > 2 else None
    slots = blocks.shape[0] - 1
    if first_call:
        blocks[slots] = jnp.zeros(blocks.shape[1:], blocks.dtype)
        total[...] = jnp.zeros(total.shape, total.dtype)
    for way in range(ways if arrived else 0):
        top = 0
        for part in parts[way * arrived // ways : (way + 1) * arrived // ways]:
            rows = part.shape[1]
            blocks[base + way, top : top + rows] = part[0]
            top += rows
    run_jobs(call, calls, table, coupling, blocks, total)
    if send is not None:
        for i, k in enumerate(sends):
            send[i] = (total[k] * scale).astype(send.dtype)


def finish_kernel(call, calls, scale, table, part_ref, coupling, blocks, total_in, total, out, ready, done):
    run_jobs(call, calls, table, coupling, blocks, total, wide=True)
    local = ready.shape[0]
    copies = []
    for k in range(local):
        ready[k] = total[local + k] * scale
        copies.append(pltpu.make_async_copy(ready.at[k], out.at[k, 0, part_ref[0]], done.at[k]))
        copies[k].start()
    for copy in copies:
        copy.wait()


def write_other_kernel(at, part_ref, *refs):
    parts, (out, ready, done) = refs[:-4], refs[-3:]
    copies = []
    for k, part in enumerate(parts):
        ready[k] = part[0].astype(ready.dtype)
        place = out.at[at + k, 0, part_ref[0]]
        copies.append(pltpu.make_async_copy(ready.at[k], place, done.at[k]))
        copies[k].start()
    for copy in copies:
        copy.wait()


def solution(mesh):
    moms, energies = mesh.shape["mom"], mesh.shape["en"]
    bits = moms.bit_length() - 2
    top = moms // 2
    both = ("mom", "en")

    def move(value, target):
        pairs = []
        for m in range(moms):
            for e in range(energies):
                to_m, to_e = target(m, e)
                if not 0 <= to_e < energies:
                    to_m, to_e = m, e ^ 1
                pairs.append((m * energies + e, to_m * energies + to_e))
        return lax.ppermute(value, both, pairs)

    def away(m, e):
        return m, e + (2 if e % 2 else -2)

    def toward(m, e):
        return m, e + (-2 if e % 2 else 2)

    def core_mate(m, e):
        return m, e ^ 1

    def partner(m, e):
        return m ^ (top if e % 2 else 1), e

    def gather_bit(bit):
        return lambda m, e: (m ^ ((1 << bit) if e % 2 else (2 << bit)), e)

    def body(green_blocks, transfer_index, photon_shift, photon_occupancy, coupling):
        local, _, parts, orbitals, _ = green_blocks.shape
        momenta = transfer_index.shape[1]
        classes = coupling.shape[0]
        ways = 1 << bits
        slots = 2 * local * ways
        last = 2 * local - 1
        calls = last + local + 3
        low = jnp.bfloat16
        scale = 1.0 / momenta
        m, e = lax.axis_index("mom"), lax.axis_index("en")
        even = e % 2 == 0
        bit_of = (m & 1, (m // top) & 1)
        mine = jnp.where(even, bit_of[0], bit_of[1])
        mates = jnp.where(even, bit_of[1], bit_of[0])
        flat = green_blocks.reshape(local, parts, orbitals, orbitals)
        block_shape = (orbitals, orbitals)
        smem = pl.BlockSpec(memory_space=pltpu.SMEM)
        vmem = pl.BlockSpec(memory_space=pltpu.VMEM)
        product = 4 * orbitals**3
        pieces = pieces_of(local)

        def kernel(act, *args, flops=1 << 20, vmem_mib=8, **more):
            return pl.pallas_call(
                act,
                compiler_params=pltpu.CompilerParams(vmem_limit_bytes=vmem_mib * MIB),
                cost_estimate=pl.CostEstimate(flops=flops, bytes_accessed=MIB, transcendentals=0),
                **more,
            )(*args)

        def send(value, target):
            came = move(value, target)
            if value.dtype != low:
                return came
            return pltpu.with_memory_space_constraint(came, pltpu.VMEM)

        place = jnp.stack(
            [m, jnp.where(even, 1, top)]
            + [jnp.where(even, 2 << bit, 1 << bit) for bit in range(bits)]
        ).astype(jnp.int32)
        has_below, has_above = e >= 2, e + 2 < energies
        sides = jnp.stack(
            [even, jnp.where(even, has_below, has_above), jnp.where(even, has_above, has_below)]
        ).astype(jnp.int32)
        which = jnp.stack([mine, 1 - mine, mates, 1 - mates]).astype(jnp.int32)
        place, sides, which = lax.optimization_barrier((place, sides, which))
        packed = transfer_index + classes * photon_shift[:, None]
        partner_index = send(packed, partner)

        flat = pltpu.with_memory_space_constraint(flat, pltpu.HBM)
        near_unit = pltpu.VMEM((1, *block_shape), low)
        near_units = pltpu.VMEM((local, *block_shape), low)
        weight_count = pltpu.SMEM((1 + 2 * local,), jnp.float32)
        first = kernel(
            convert_first_kernel,
            which,
            flat,
            grid_spec=pltpu.PrefetchScalarGridSpec(
                num_scalar_prefetch=1,
                grid=(1,),
                in_specs=[pl.BlockSpec((1, 1, *block_shape), lambda i, p: (0, p[0], 0, 0))],
                out_specs=vmem,
            ),
            out_shape=near_unit,
        )
        *rounded, own_weights, flags = kernel(
            functools.partial(convert_kernel, local),
            which,
            photon_shift,
            photon_occupancy,
            sides,
            flat,
            grid_spec=pltpu.PrefetchScalarGridSpec(
                num_scalar_prefetch=1,
                grid=(local,),
                in_specs=[smem] * 3
                + [pl.BlockSpec((1, parts, *block_shape), lambda i, p: (i, 0, 0, 0))],
                out_specs=[vmem] * (local + 1) + [smem] * 2,
            ),
            out_shape=[near_unit] * (local - 1)
            + [near_units, pltpu.VMEM((2 * local, *block_shape), low)]
            + [weight_count, pltpu.SMEM((local,), jnp.int32)],
        )
        own, (others, mates_blocks) = [first, *rounded[: local - 1]], rounded[local - 1 :]
        mate = send(mates_blocks, core_mate)
        ready = kernel(
            functools.partial(choose_kernel, local),
            flags,
            mate,
            *own,
            others,
            in_specs=[smem] + [vmem] * (2 + local),
            out_specs=[vmem] * sum(pieces),
            out_shape=[
                pltpu.VMEM((1, orbitals // n, orbitals), low) for n in pieces for _ in range(n)
            ],
        )
        ready = list(ready)
        ready = [[ready.pop(0) for _ in range(n)] for n in pieces]

        def sends(values, target):
            return [send(value, target) for value in values]

        gone = [sends([own[k]], away) for k in range(local)]
        chosen = ready[:local]
        chosen += [sends(ready[k], partner) for k in range(local, 2 * local)]
        gone += [sends(chosen[k], away) for k in range(local, 2 * local)]
        came = [sends(value, toward) for value in chosen]
        bins = 2 * local * classes
        room = calls + calls * 2 * local * momenta * FIELDS
        table, partner_weights = kernel(
            functools.partial(plan_kernel, (local, momenta, classes, bits, calls)),
            packed,
            partner_index,
            photon_occupancy,
            sides,
            place,
            in_specs=[smem] * 5,
            out_specs=[smem] * 2,
            out_shape=[pltpu.SMEM((room,), jnp.int32), weight_count],
            scratch_shapes=[
                pltpu.SMEM((bins,), jnp.int32),
                pltpu.SMEM((bins * slots,), jnp.int32),
                pltpu.SMEM((calls,), jnp.int32),
            ],
        )

        stages = [
            [
                kernel(
                    functools.partial(mix_kernel, k % local, local),
                    own_weights if k < local else partner_weights,
                    came[k][i],
                    chosen[k][i],
                    gone[k][i],
                    in_specs=[smem] + [vmem] * 3,
                    out_specs=vmem,
                    out_shape=pltpu.VMEM(came[k][i].shape, low),
                )
                for i in range(pieces[k])
            ]
            for k in range(2 * local)
        ]

        weights = pltpu.with_memory_space_constraint(coupling, pltpu.VMEM)
        out_state = [
            pltpu.VMEM((slots + 1, *block_shape), low),
            pltpu.VMEM((2 * local, *block_shape), jnp.float32),
        ]

        def stage(call, arrived, state, sends, jobs, base=0):
            given = [] if state is None else list(state)
            result = kernel(
                functools.partial(stage_kernel, call, calls, base, ways, len(arrived), sends, scale),
                table,
                weights,
                *arrived,
                *given,
                flops=jobs * product,
                vmem_mib=12,
                in_specs=[smem, vmem] + [vmem] * (len(arrived) + len(given)),
                out_specs=[vmem] * (2 + bool(sends)),
                out_shape=out_state + [pltpu.VMEM((len(sends), *block_shape), low)] * bool(sends),
                input_output_aliases={2 + len(arrived) + i: i for i in range(len(given))},
            )
            return result[:2], result[2:]

        state = None
        got = []
        for call, held in enumerate(stages):
            arrived = [held]
            for bit in range(bits):
                for values in list(arrived):
                    arrived.append(sends(values, gather_bit(bit)))
            arrived = [piece for values in arrived for piece in values]
            sends_now = [0] if call == last else []
            if call == last - 1:
                state, _ = stage(last, [], state, [], 3)
            state, sent = stage(call + 2 * (call == last), arrived, state, sends_now, 5, call * ways)
        got = []
        for k in range(local):
            if k:
                state, sent = stage(last + 2 + k, [], state, [k], 2)
            got.append(send(sent[0], partner))
        state, _ = stage(last + 1, [], state, [], 5)

        hbm = pl.BlockSpec(memory_space=pltpu.HBM)
        out_shape = jax.ShapeDtypeStruct(green_blocks.shape, jnp.float32)
        staging = [
            pltpu.VMEM((local, *block_shape), jnp.float32),
            pltpu.SemaphoreType.DMA((local,)),
        ]
        _, result = kernel(
            functools.partial(finish_kernel, last + 2 + local, calls, scale),
            table,
            mine.reshape(1),
            weights,
            *state,
            vmem_mib=14,
            in_specs=[smem] * 2 + [vmem] * 3,
            out_specs=[vmem, hbm],
            out_shape=[out_state[1], out_shape],
            input_output_aliases={4: 0},
            scratch_shapes=staging,
        )
        for name, values in (("early", got[:-1]), ("last", got[-1:])):
            result = kernel(
                functools.partial(write_other_kernel, 0 if name == "early" else local - 1),
                (1 - mine).reshape(1),
                *values,
                result,
                in_specs=[smem] + [vmem] * len(values) + [hbm],
                out_specs=hbm,
                out_shape=out_shape,
                input_output_aliases={1 + len(values): 0},
                scratch_shapes=staging,
            )
        return result

    placed = (P("mom", "en", None, None, None), P("mom", None), P("mom"), P(), P())

    return jax.shard_map(
        body,
        mesh=mesh,
        in_specs=placed,
        out_specs=P("mom", "en", None, None, None),
        check_vma=False,
    )
```

```python
import functools

import jax
import jax.numpy as jnp
from jax import lax
from jax.experimental import pallas as pl
from jax.experimental.pallas import tpu as pltpu
from jax.sharding import PartitionSpec as P


MEMBERS = 4
FIELDS = 8
SIZES = (4, 2, 1)
MIB = 1 << 20
LAST_ROWS = (((1,), (1,)), ((), ()))


def pieces_of(local):
    return [1] * (2 * local - 1) + [2]


def settle(near, occupancy, place, weights):
    local = len(near)
    occupy = occupancy[0]
    even, has_toward, has_away = place[0] == 1, place[1] == 1, place[2] == 1
    weights[0] = jnp.where(has_toward, jnp.where(even, occupy, occupy + 1.0), 0.0)
    heavy = jnp.where(even, occupy + 1.0, occupy)
    for k in range(local):
        weights[1 + k] = jnp.where(near[k], heavy, 0.0)
        weights[1 + local + k] = jnp.where(near[k] | jnp.logical_not(has_away), 0.0, heavy)


def plan_kernel(sizes, own_ref, partner_ref, occupancy, sides, place_ref, table, weights, count, member, filled):
    local, momenta, classes, bits, calls = sizes
    ways = 1 << bits
    slots = 2 * local * ways
    bins = 2 * local * classes
    room = 2 * local * momenta
    near = [lax.div(partner_ref[k, 0], classes) == 1 for k in range(local)]
    settle(near, occupancy, sides, weights)

    for index in range(bins):
        count[index] = 0
    for call in range(calls):
        filled[call] = 0
        table[call] = 0

    def sort_slot(slot, _):
        stage = lax.div(slot, ways)
        way = lax.rem(slot, ways)
        home = place_ref[0]
        for bit in range(bits):
            home = home ^ jnp.where((way >> bit) & 1 == 1, place_ref[2 + bit], 0)
        home = home ^ jnp.where(stage < local, 0, place_ref[1])
        momentum = home * local + lax.rem(stage, local)
        for k in range(2 * local):
            of_k = partner_ref[k, momentum] if k < local else own_ref[k - local, momentum]
            of_k = lax.rem(of_k, classes)
            index = k * classes + of_k
            have = count[index]
            member[index * slots + have] = slot
            count[index] = have + 1
        return 0

    lax.fori_loop(0, slots, sort_slot, 0)

    for k in range(2 * local):

        def one_bin(q, _):
            index = k * classes + q
            have = count[index]

            def one_job(j, _):
                first = index * slots + j * MEMBERS
                upto = jnp.minimum(MEMBERS, have - j * MEMBERS)
                last = 2 * local - 1
                latest = member[first + upto - 1]
                stage = jnp.where(latest == last * ways, last - 1, lax.div(latest, ways))
                if k < local:
                    call = jnp.where(stage == last, last + k, stage)
                else:
                    call = jnp.where(stage < last - 2, stage, last + local)
                place = filled[call]
                filled[call] = place + 1
                table[call] = place + 1
                at = calls + (call * room + place) * FIELDS
                table[at] = k
                table[at + 1] = q
                for i in range(MEMBERS):
                    table[at + 2 + i] = jnp.where(i < upto, member[first + i], slots)
                return 0

            return lax.fori_loop(0, lax.div(have + MEMBERS - 1, MEMBERS), one_job, 0)

        lax.fori_loop(0, classes, one_bin, 0)


def convert_first_kernel(part_ref, block, out):
    out[0] = block[0, 0].astype(out.dtype)


def convert_kernel(local, part_ref, shift, occupancy, sides, block, *outs):
    step = pl.program_id(0)
    low = outs[0].dtype
    weights, flags = outs[-2:]

    @pl.when(step == 0)
    def _():
        near = [shift[k] == 1 for k in range(local)]
        settle(near, occupancy, sides, weights)
        for k in range(local):
            flags[k] = jnp.where(near[k], 1, 0)

    for k in range(1, local):

        @pl.when(step == k)
        def _():
            outs[k - 1][0] = block[0, part_ref[0]].astype(low)

    outs[local - 1][step] = block[0, part_ref[1]].astype(low)
    outs[local][step] = block[0, part_ref[2]].astype(low)
    outs[local][local + step] = block[0, part_ref[3]].astype(low)


def choose_kernel(local, flags, mate, *refs):
    own, others, outs = refs[:local], refs[local], list(refs[local + 1 :])
    for k, cuts in enumerate(pieces_of(local)):
        rows = mate.shape[1] // cuts
        given, at = (own[k], 0) if k < local else (others, k - local)
        near = flags[k % local] == 1
        for top in range(0, mate.shape[1], rows):
            out = outs.pop(0)

            @pl.when(near)
            def _():
                out[0] = mate[k, top : top + rows]

            @pl.when(jnp.logical_not(near))
            def _():
                out[0] = given[at, top : top + rows]


def mix_kernel(k, local, weights, came, chosen, gone, out):
    wide = jnp.float32
    out[...] = (
        weights[0] * came[...].astype(wide)
        + (
            weights[1 + k] * chosen[...].astype(wide)
            + weights[1 + local + k] * gone[...].astype(wide)
        )
    ).astype(out.dtype)


def run_jobs(call, calls, table, coupling, blocks, total, wide=False):
    header = calls + call * ((table.shape[0] - calls) // calls)

    def step(i, _, first, jobs):
        for u in range(jobs):
            at = header + (first + i * jobs + u) * FIELDS
            k, q = table[at], table[at + 1]
            summed = blocks[table[at + 2]].astype(jnp.float32)
            for j in range(1, MEMBERS):
                summed = summed + blocks[table[at + 2 + j]].astype(jnp.float32)
            weight = coupling[q]
            left = jnp.dot(weight, summed.astype(blocks.dtype), preferred_element_type=jnp.float32)
            total[k] += lax.dot_general(
                left.astype(blocks.dtype), weight, LAST_ROWS, preferred_element_type=jnp.float32
            )
        return 0

    done, jobs = 0, table[call]
    for size in SIZES[0 if wide else 1 :]:
        count = lax.div(jobs - done, size)
        lax.fori_loop(0, count, functools.partial(step, first=done, jobs=size), 0)
        done = done + count * size


def stage_kernel(call, calls, layout, arrived, sends, scale, table, coupling, *refs):
    parts = refs[:arrived]
    first_call = call == 0
    refs = refs[arrived:] if first_call else refs[arrived + 2 :]
    blocks, total = refs[:2]
    send = refs[2] if len(refs) > 2 else None
    slots = blocks.shape[0] - 1
    if first_call:
        blocks[slots] = jnp.zeros(blocks.shape[1:], blocks.dtype)
        total[...] = jnp.zeros(total.shape, total.dtype)
    parts = list(parts)
    for slot, cuts in layout:
        top = 0
        for _ in range(cuts):
            part = parts.pop(0)
            blocks[slot, top : top + part.shape[1]] = part[0]
            top += part.shape[1]
    run_jobs(call, calls, table, coupling, blocks, total, wide=len(layout) > 2)
    if send is not None:
        for i, k in enumerate(sends):
            send[i] = (total[k] * scale).astype(send.dtype)


def finish_kernel(call, calls, scale, table, part_ref, coupling, blocks, total_in, total, out, ready, done):
    run_jobs(call, calls, table, coupling, blocks, total, wide=True)
    local = ready.shape[0]
    copies = []
    for k in range(local):
        ready[k] = total[local + k] * scale
        copies.append(pltpu.make_async_copy(ready.at[k], out.at[k, 0, part_ref[0]], done.at[k]))
        copies[k].start()
    for copy in copies:
        copy.wait()


def write_other_kernel(at, part_ref, *refs):
    parts, (out, ready, done) = refs[:-4], refs[-3:]
    copies = []
    for k, part in enumerate(parts):
        ready[k] = part[0].astype(ready.dtype)
        place = out.at[at + k, 0, part_ref[0]]
        copies.append(pltpu.make_async_copy(ready.at[k], place, done.at[k]))
        copies[k].start()
    for copy in copies:
        copy.wait()


def solution(mesh):
    moms, energies = mesh.shape["mom"], mesh.shape["en"]
    bits = moms.bit_length() - 2
    top = moms // 2
    both = ("mom", "en")

    def move(value, target):
        pairs = []
        for m in range(moms):
            for e in range(energies):
                to_m, to_e = target(m, e)
                if not 0 <= to_e < energies:
                    to_m, to_e = m, e ^ 1
                pairs.append((m * energies + e, to_m * energies + to_e))
        return lax.ppermute(value, both, pairs)

    def away(m, e):
        return m, e + (2 if e % 2 else -2)

    def toward(m, e):
        return m, e + (-2 if e % 2 else 2)

    def core_mate(m, e):
        return m, e ^ 1

    def partner(m, e):
        return m ^ (top if e % 2 else 1), e

    def gather_bit(bit):
        return lambda m, e: (m ^ ((1 << bit) if e % 2 else (2 << bit)), e)

    def body(green_blocks, transfer_index, photon_shift, photon_occupancy, coupling):
        local, _, parts, orbitals, _ = green_blocks.shape
        momenta = transfer_index.shape[1]
        classes = coupling.shape[0]
        ways = 1 << bits
        slots = 2 * local * ways
        last = 2 * local - 1
        calls = last + local + 1
        low = jnp.bfloat16
        scale = 1.0 / momenta
        m, e = lax.axis_index("mom"), lax.axis_index("en")
        even = e % 2 == 0
        bit_of = (m & 1, (m // top) & 1)
        mine = jnp.where(even, bit_of[0], bit_of[1])
        mates = jnp.where(even, bit_of[1], bit_of[0])
        flat = green_blocks.reshape(local, parts, orbitals, orbitals)
        block_shape = (orbitals, orbitals)
        smem = pl.BlockSpec(memory_space=pltpu.SMEM)
        vmem = pl.BlockSpec(memory_space=pltpu.VMEM)
        product = 4 * orbitals**3
        pieces = pieces_of(local)

        def kernel(act, *args, flops=1 << 20, vmem_mib=8, **more):
            return pl.pallas_call(
                act,
                compiler_params=pltpu.CompilerParams(vmem_limit_bytes=vmem_mib * MIB),
                cost_estimate=pl.CostEstimate(flops=flops, bytes_accessed=MIB, transcendentals=0),
                **more,
            )(*args)

        def send(value, target):
            came = move(value, target)
            if value.dtype != low:
                return came
            return pltpu.with_memory_space_constraint(came, pltpu.VMEM)

        place = jnp.stack(
            [m, jnp.where(even, 1, top)]
            + [jnp.where(even, 2 << bit, 1 << bit) for bit in range(bits)]
        ).astype(jnp.int32)
        has_below, has_above = e >= 2, e + 2 < energies
        sides = jnp.stack(
            [even, jnp.where(even, has_below, has_above), jnp.where(even, has_above, has_below)]
        ).astype(jnp.int32)
        which = jnp.stack([mine, 1 - mine, mates, 1 - mates]).astype(jnp.int32)
        place, sides, which = lax.optimization_barrier((place, sides, which))
        packed = transfer_index + classes * photon_shift[:, None]
        partner_index = send(packed, partner)

        flat = pltpu.with_memory_space_constraint(flat, pltpu.HBM)
        near_unit = pltpu.VMEM((1, *block_shape), low)
        near_units = pltpu.VMEM((local, *block_shape), low)
        weight_count = pltpu.SMEM((1 + 2 * local,), jnp.float32)
        first = kernel(
            convert_first_kernel,
            which,
            flat,
            grid_spec=pltpu.PrefetchScalarGridSpec(
                num_scalar_prefetch=1,
                grid=(1,),
                in_specs=[pl.BlockSpec((1, 1, *block_shape), lambda i, p: (0, p[0], 0, 0))],
                out_specs=vmem,
            ),
            out_shape=near_unit,
        )
        *rounded, own_weights, flags = kernel(
            functools.partial(convert_kernel, local),
            which,
            photon_shift,
            photon_occupancy,
            sides,
            flat,
            grid_spec=pltpu.PrefetchScalarGridSpec(
                num_scalar_prefetch=1,
                grid=(local,),
                in_specs=[smem] * 3
                + [pl.BlockSpec((1, parts, *block_shape), lambda i, p: (i, 0, 0, 0))],
                out_specs=[vmem] * (local + 1) + [smem] * 2,
            ),
            out_shape=[near_unit] * (local - 1)
            + [near_units, pltpu.VMEM((2 * local, *block_shape), low)]
            + [weight_count, pltpu.SMEM((local,), jnp.int32)],
        )
        own, (others, mates_blocks) = [first, *rounded[: local - 1]], rounded[local - 1 :]
        mate = send(mates_blocks, core_mate)
        ready = kernel(
            functools.partial(choose_kernel, local),
            flags,
            mate,
            *own,
            others,
            in_specs=[smem] + [vmem] * (2 + local),
            out_specs=[vmem] * sum(pieces),
            out_shape=[
                pltpu.VMEM((1, orbitals // n, orbitals), low) for n in pieces for _ in range(n)
            ],
        )
        ready = list(ready)
        ready = [[ready.pop(0) for _ in range(n)] for n in pieces]

        def sends(values, target):
            return [send(value, target) for value in values]

        gone = [sends([own[k]], away) for k in range(local)]
        chosen = ready[:local]
        chosen += [sends(ready[k], partner) for k in range(local, 2 * local)]
        gone += [sends(chosen[k], away) for k in range(local, 2 * local)]
        came = [sends(value, toward) for value in chosen]
        bins = 2 * local * classes
        room = calls + calls * 2 * local * momenta * FIELDS
        table, partner_weights = kernel(
            functools.partial(plan_kernel, (local, momenta, classes, bits, calls)),
            packed,
            partner_index,
            photon_occupancy,
            sides,
            place,
            in_specs=[smem] * 5,
            out_specs=[smem] * 2,
            out_shape=[pltpu.SMEM((room,), jnp.int32), weight_count],
            scratch_shapes=[
                pltpu.SMEM((bins,), jnp.int32),
                pltpu.SMEM((bins * slots,), jnp.int32),
                pltpu.SMEM((calls,), jnp.int32),
            ],
        )

        stages = [
            [
                kernel(
                    functools.partial(mix_kernel, k % local, local),
                    own_weights if k < local else partner_weights,
                    came[k][i],
                    chosen[k][i],
                    gone[k][i],
                    in_specs=[smem] + [vmem] * 3,
                    out_specs=vmem,
                    out_shape=pltpu.VMEM(came[k][i].shape, low),
                )
                for i in range(pieces[k])
            ]
            for k in range(2 * local)
        ]

        weights = pltpu.with_memory_space_constraint(coupling, pltpu.VMEM)
        out_state = [
            pltpu.VMEM((slots + 1, *block_shape), low),
            pltpu.VMEM((2 * local, *block_shape), jnp.float32),
        ]

        def stage(call, arrived, state, sends, jobs, layout=()):
            given = [] if state is None else list(state)
            result = kernel(
                functools.partial(stage_kernel, call, calls, layout, len(arrived), sends, scale),
                table,
                weights,
                *arrived,
                *given,
                flops=jobs * product,
                vmem_mib=12,
                in_specs=[smem, vmem] + [vmem] * (len(arrived) + len(given)),
                out_specs=[vmem] * (2 + bool(sends)),
                out_shape=out_state + [pltpu.VMEM((len(sends), *block_shape), low)] * bool(sends),
                input_output_aliases={2 + len(arrived) + i: i for i in range(len(given))},
            )
            return result[:2], result[2:]

        state = None
        got = []
        for call, held in enumerate(stages):
            arrived = [held]
            for bit in range(bits):
                for values in list(arrived):
                    arrived.append(sends(values, gather_bit(bit)))
            places = [call * ways + way for way in range(ways)]
            if call == last - 1:
                arrived, places = [*arrived, stages[last]], [*places, last * ways]
            if call == last:
                arrived, places = arrived[1:], places[1:]
            layout = [(place, len(values)) for place, values in zip(places, arrived)]
            arrived = [piece for values in arrived for piece in values]
            sends_now = [0] if call == last else []
            state, sent = stage(call, arrived, state, sends_now, 5, layout)
        for k in range(local):
            if k:
                state, sent = stage(last + k, [], state, [k], 2)
            got.append(send(sent[0], partner))

        hbm = pl.BlockSpec(memory_space=pltpu.HBM)
        out_shape = jax.ShapeDtypeStruct(green_blocks.shape, jnp.float32)
        staging = [
            pltpu.VMEM((local, *block_shape), jnp.float32),
            pltpu.SemaphoreType.DMA((local,)),
        ]
        _, result = kernel(
            functools.partial(finish_kernel, last + local, calls, scale),
            table,
            mine.reshape(1),
            weights,
            *state,
            vmem_mib=14,
            in_specs=[smem] * 2 + [vmem] * 3,
            out_specs=[vmem, hbm],
            out_shape=[out_state[1], out_shape],
            input_output_aliases={4: 0},
            scratch_shapes=staging,
        )
        for name, values in (("early", got[:-1]), ("last", got[-1:])):
            result = kernel(
                functools.partial(write_other_kernel, 0 if name == "early" else local - 1),
                (1 - mine).reshape(1),
                *values,
                result,
                in_specs=[smem] + [vmem] * len(values) + [hbm],
                out_specs=hbm,
                out_shape=out_shape,
                input_output_aliases={1 + len(values): 0},
                scratch_shapes=staging,
            )
        return result

    placed = (P("mom", "en", None, None, None), P("mom", None), P("mom"), P(), P())

    return jax.shard_map(
        body,
        mesh=mesh,
        in_specs=placed,
        out_specs=P("mom", "en", None, None, None),
        check_vma=False,
    )
```
